16 devices in a mesh: data: 2 (over y, z), time: 8 (over x, core).
Axes of the slice: x: 4, y: 2, z: 1, core: 2. Of those that a mesh axis runs over, the one named last changes fastest.
The devices are a block of a 4x4x8 slice.
Arguments:
- x_init: float32 [8, 256, 16], P('data'), parts along dimension 0
- w_in: bfloat16 [16, 768], replicated
- w_out: bfloat16 [768, 16], replicated
- mod_scale: bfloat16 [24, 768], P('time')
- mod_shift: bfloat16 [24, 768], P('time')
- step_size: float32 [24], P('time')
Outputs:
- output: float32 [24, 8, 256, 16], P('time', 'data'), parts along dimension 1
There are 2 independent parts. The reference program is written for one: setup_inputs(seed, part) draws one part's arguments, and reference() takes and returns one part's arrays. A program takes and returns all parts, laid end to end along the dimension named above; an argument that names none is the same for every part.
All inputs are finite; a program needn't handle non-finite values.
Results may differ from the reference program's by a relative error of at most 0.001.
Values are sent between devices in bfloat16 or wider.
A program may use at most 768 MiB of HBM per device.

```python
import jax
import jax.numpy as jnp
from jax import lax

TOKENS = 256
CHANNELS = 16
HIDDEN = 768
STEPS_DEV = 3
BATCH = 4
TIME_DEVS = 8
SWEEPS = 4


def setup_inputs(seed: int = 0, part: int = 0) -> dict:
    total_steps = TIME_DEVS * STEPS_DEV
    keys = jax.random.split(jax.random.key(seed), 6)
    x_init = jax.random.normal(jax.random.fold_in(keys[0], part), (BATCH, TOKENS, CHANNELS), jnp.float32)
    w_in = jax.random.normal(keys[1], (CHANNELS, HIDDEN), jnp.float32) * (CHANNELS * total_steps) ** -0.5
    w_raw = jax.random.normal(keys[2], (HIDDEN, CHANNELS), jnp.float32)
    w_out = (w_raw - jnp.mean(w_raw, axis=0, keepdims=True)) * HIDDEN ** -0.5
    mod_scale = 0.5 * jax.random.normal(keys[3], (total_steps, HIDDEN), jnp.float32)
    mod_shift = jax.random.normal(keys[4], (total_steps, HIDDEN), jnp.float32)
    step_size = jax.random.uniform(keys[5], (total_steps,), jnp.float32, 0.5, 1.5) * (2.5 * total_steps ** -0.5)
    return {'x_init': x_init, 'w_in': w_in.astype(jnp.bfloat16), 'w_out': w_out.astype(jnp.bfloat16), 'mod_scale': mod_scale.astype(jnp.bfloat16), 'mod_shift': mod_shift.astype(jnp.bfloat16), 'step_size': step_size}


def drift_block(latent, scale_rows, shift_rows, step_rows, w_in, w_out):
    x_rounded = latent.astype(jnp.bfloat16).astype(jnp.float32)
    pre_act = jnp.einsum('kbnc,cd->kbnd', x_rounded, w_in.astype(jnp.float32))
    gain_rows = 1.0 + scale_rows.astype(jnp.float32)
    hidden = jax.nn.gelu(pre_act * gain_rows[:, None, None, :] + shift_rows.astype(jnp.float32)[:, None, None, :], approximate=True)
    out_act = jnp.einsum('kbnd,dc->kbnc', hidden.astype(jnp.bfloat16).astype(jnp.float32), w_out.astype(jnp.float32))
    return step_rows[:, None, None, None] * out_act


def reference(x_init, w_in, w_out, mod_scale, mod_shift, step_size):
    total_steps = TIME_DEVS * STEPS_DEV
    lat_shape = (BATCH, TOKENS, CHANNELS)
    scale_blocks = mod_scale.reshape(TIME_DEVS, STEPS_DEV, HIDDEN)
    shift_blocks = mod_shift.reshape(TIME_DEVS, STEPS_DEV, HIDDEN)
    step_blocks = step_size.reshape(TIME_DEVS, STEPS_DEV)

    def one_block(block):
        return drift_block(block[0], block[1], block[2], block[3], w_in, w_out)

    def one_sweep(sweep_idx, latent):
        lat_blocks = latent.reshape((TIME_DEVS, STEPS_DEV) + lat_shape)
        drifts = lax.map(one_block, (lat_blocks, scale_blocks, shift_blocks, step_blocks))
        drifts = drifts.reshape((total_steps,) + lat_shape)
        inclusive = jnp.cumsum(drifts, axis=0)
        exclusive = jnp.concatenate([jnp.zeros_like(drifts[:1]), inclusive[:-1]], axis=0)
        return x_init[None] + exclusive

    start = jnp.broadcast_to(x_init[None], (total_steps,) + lat_shape)
    return lax.fori_loop(0, SWEEPS, one_sweep, start)
```

```python
import functools

import jax
import jax.numpy as jnp
from jax import lax
from jax.experimental import pallas as pl
from jax.experimental.pallas import tpu as pltpu
from jax.sharding import PartitionSpec as P

SWEEPS = 4
F32, BF16 = jnp.float32, jnp.bfloat16
MESH = pl.DeviceIdType.MESH
LIN = 2 * 0.7978845608028654
CUB = 8 * 0.7978845608028654 * 0.044715


def kernel(n, x_ref, w_in_ref, w_out_ref, scale_ref, shift_ref, step_ref, out_ref,
           mods, first, first_send, lat, final, pre, mod_send, mod_recv, f_send, f_recv, o_send, o_recv):
    me = lax.axis_index("time")
    steps = scale_ref.shape[0]
    total = n * steps
    samples, chans, tokens = x_ref.shape
    hidden = w_in_ref.shape[1]
    width = samples * tokens // n
    per = tokens // width
    chips = n // per

    barrier = pltpu.get_barrier_semaphore()
    for d in range(1, n):
        pl.semaphore_signal(barrier, inc=1, device_id={"time": lax.rem(me + d, n)}, device_id_type=MESH)

    def place(dev):
        return dev // per, pl.ds(pl.multiple_of(lax.rem(dev, per) * width, width), width)

    for k in range(steps):
        mods[me, k:k + 1, :] = 0.5 * (1.0 + scale_ref[k:k + 1, :].astype(F32))
        mods[me, steps + k:steps + k + 1, :] = 0.5 * shift_ref[k:k + 1, :].astype(F32)
        mods[me, 2 * steps:2 * steps + 1, k * width:(k + 1) * width] = jnp.full((1, width), step_ref[k], F32)

    w_in = w_in_ref[...]
    w_out = w_out_ref[...]

    def up(slot, xt):
        pre[slot] = lax.dot_general(xt.astype(BF16), w_in, (((0,), (0,)), ((), ())), preferred_element_type=F32)

    def act(p, gain, shift):
        v = p * gain + shift
        return v + v * jnp.tanh(v * (v * v * CUB + LIN))

    def down(h):
        return lax.dot_general(w_out, h.astype(BF16), (((1,), (1,)), ((), ())), preferred_element_type=F32)

    pl.semaphore_wait(barrier, n - 1)
    mod_copies = []
    for d in range(1, n):
        dst = lax.rem(me + d, n)
        src = lax.rem(me + n - d, n)
        copy = pltpu.make_async_remote_copy(mods.at[me], mods.at[me], mod_send.at[d], mod_recv.at[d], device_id={"time": dst}, device_id_type=MESH)
        copy.start()
        mod_copies.append((copy, pltpu.make_async_remote_copy(mods.at[me], mods.at[src], mod_send.at[d], mod_recv.at[d], device_id={"time": dst}, device_id_type=MESH)))

    ring = sorted(range(chips), key=lambda d: -min(d, chips - d))
    f_copies = []
    my_chip = me // per
    up(0, x_ref[lax.rem(my_chip + ring[0], chips)])
    for i, d in enumerate(ring):
        chip = lax.rem(my_chip + d, chips)
        if i + 1 < chips:
            up((i + 1) % 2, x_ref[lax.rem(my_chip + ring[i + 1], chips)])
        p = pre[i % 2]
        for k in range(steps):
            f = down(act(p, mods[me, k:k + 1, :], mods[me, steps + k:steps + k + 1, :])) * step_ref[k]
            for c in range(per):
                first_send[chip * per + c, k] = f[:, c * width:(c + 1) * width]
        for c in range(per):
            if d == 0 and c == 0:
                first[me] = first_send[me]
                continue
            dst = chip * per + c if d else chip * per + lax.rem(lax.rem(me, per) + c, per)
            idx = d * per + c
            copy = pltpu.make_async_remote_copy(first_send.at[dst], first.at[me], f_send.at[idx], f_recv.at[me], device_id={"time": dst}, device_id_type=MESH)
            copy.start()
            f_copies.append(copy)

    for copy, arrival in mod_copies:
        copy.wait_send()
        arrival.wait_recv()
    for copy in f_copies:
        copy.wait_send()
    for d in range(1, n):
        src = lax.rem(me + d, n)
        pltpu.make_async_remote_copy(first_send.at[src], first.at[src], f_send.at[d], f_recv.at[src], device_id={"time": src}, device_id_type=MESH).wait_recv()

    mine_b, mine_l = place(me)
    x_mine = x_ref[mine_b, :, mine_l]

    def row(j, r):
        return mods[j // steps, r:r + 1, :]

    def drift_steps(j):
        k = j % steps
        return mods[j // steps, 2 * steps:2 * steps + 1, k * width:(k + 1) * width]

    run = x_mine + first[0, 0]
    for s in range(SWEEPS - 1):
        lat[s, 1] = run
    for j in range(1, total - 1):
        run = run + first[j // steps, j % steps]
        lat[0, j + 1] = run

    def pairs(s, todo):
        def load(j):
            return jnp.concatenate([lat[s, j], lat[s, j + 1]], axis=1)
        up(0, load(todo[0]))
        for i, j in enumerate(todo):
            if i + 1 < len(todo):
                up((i + 1) % 2, load(todo[i + 1]))
            p = pre[i % 2]
            h = []
            for c in range(2):
                k = (j + c) % steps
                h.append(act(p[c * width:(c + 1) * width], row(j + c, k), row(j + c, steps + k)))
            f = down(jnp.concatenate(h, axis=0))
            for c in range(2):
                prev = lat[s + 1, j + c] if s + 1 < SWEEPS - 1 else final[(j + c) // steps, (j + c) % steps]
                nxt = prev + f[:, c * width:(c + 1) * width] * drift_steps(j + c)
                if s + 1 < SWEEPS - 1:
                    lat[s + 1, j + c + 1] = nxt
                else:
                    final[(j + c + 1) // steps, (j + c + 1) % steps] = nxt

    everything = list(range(1, total - 1, 2))
    for s in range(SWEEPS - 2):
        pairs(s, everything)

    final[0, 0] = x_mine
    for j in range(1, SWEEPS):
        final[j // steps, j % steps] = lat[SWEEPS - 2, j]

    o_copies = []

    def send(q):
        copy = pltpu.make_async_remote_copy(final.at[q], out_ref.at[:, mine_b, :, mine_l], o_send.at[q], o_recv.at[me], device_id={"time": q}, device_id_type=MESH)

        @pl.when(me != q)
        def _():
            copy.start()

        @pl.when(me == q)
        def _():
            for k in range(steps):
                out_ref[k, mine_b, :, mine_l] = final[q, k]

    rest = everything[(SWEEPS - 1) // 2:]
    sent = 0
    for part in (rest[:4], rest[4:8], rest[8:]):
        pairs(SWEEPS - 2, part)
        while sent < n and (sent + 1) * steps - 1 <= part[-1] + 2:
            send(sent)
            sent += 1
    for q in range(n):
        copy = pltpu.make_async_remote_copy(final.at[q], out_ref.at[:, q // per, :, (q % per) * width:(q % per + 1) * width], o_send.at[q], o_recv.at[q], device_id={"time": q}, device_id_type=MESH)

        @pl.when(me != q)
        def _():
            copy.wait_send()
            copy.wait_recv()


def solution(mesh):
    n = mesh.shape["time"]

    def per_device(x_init, w_in, w_out, mod_scale, mod_shift, step_size):
        samples, tokens, chans = x_init.shape
        hidden = w_in.shape[1]
        steps = step_size.shape[0]
        total = n * steps
        width = samples * tokens // n
        rows = -(-(2 * steps + 1) // 8) * 8
        vmem = pl.BlockSpec(memory_space=pltpu.VMEM)
        out = pl.pallas_call(
            functools.partial(kernel, n),
            out_shape=jax.ShapeDtypeStruct((steps, samples, chans, tokens), F32),
            in_specs=[vmem] * 5 + [pl.BlockSpec(memory_space=pltpu.SMEM)],
            out_specs=vmem,
            scratch_shapes=[
                pltpu.VMEM((n, rows, hidden), F32),
                pltpu.VMEM((n, steps, chans, width), F32),
                pltpu.VMEM((n, steps, chans, width), F32),
                pltpu.VMEM((SWEEPS - 1, total, chans, width), F32),
                pltpu.VMEM((n, steps, chans, width), F32),
                pltpu.VMEM((2, 2 * width, hidden), F32),
                pltpu.SemaphoreType.DMA((n,)),
                pltpu.SemaphoreType.DMA((n,)),
                pltpu.SemaphoreType.DMA((n,)),
                pltpu.SemaphoreType.DMA((n,)),
                pltpu.SemaphoreType.DMA((n,)),
                pltpu.SemaphoreType.DMA((n,)),
            ],
            compiler_params=pltpu.CompilerParams(collective_id=0, has_side_effects=True),
        )(jnp.transpose(x_init, (0, 2, 1)), w_in, w_out.T, mod_scale, mod_shift, step_size)
        return jnp.transpose(out, (0, 1, 3, 2))

    return jax.shard_map(per_device, mesh=mesh, in_specs=(P('data'), P(), P(), P('time'), P('time'), P('time')), out_specs=P('time', 'data'), check_vma=False)
```

```python
import functools

import jax
import jax.numpy as jnp
from jax import lax
from jax.experimental import pallas as pl
from jax.experimental.pallas import tpu as pltpu
from jax.sharding import PartitionSpec as P

SWEEPS = 4
F32, BF16 = jnp.float32, jnp.bfloat16
MESH = pl.DeviceIdType.MESH
LIN = 2 * 0.7978845608028654
CUB = 8 * 0.7978845608028654 * 0.044715


def kernel(n, x_hbm, w_in_hbm, w_out_hbm, scale_hbm, shift_hbm, step_hbm, out_ref,
           x_ref, w_in_ref, w_out_ref, rows, sizes, gains, hs, first, first_send, lat, final, pre,
           load_sem, row_send, row_recv, size_send, size_recv, f_send, f_recv, o_send, o_recv):
    me = lax.axis_index("time")
    steps = scale_hbm.shape[0]
    total = n * steps
    samples, chans, tokens = x_hbm.shape
    width = samples * tokens // n
    per = tokens // width
    chips = n // per

    barrier = pltpu.get_barrier_semaphore()
    for d in range(1, n):
        pl.semaphore_signal(barrier, inc=1, device_id={"time": lax.rem(me + d, n)}, device_id_type=MESH)

    mine_b, mine_l = me // per, pl.ds(pl.multiple_of(lax.rem(me, per) * width, width), width)
    loads = [pltpu.make_async_copy(src, dst, load_sem.at[i]) for i, (src, dst) in enumerate([
        (scale_hbm, rows.at[me, 0]), (shift_hbm, rows.at[me, 1]), (x_hbm, x_ref), (w_in_hbm, w_in_ref), (w_out_hbm, w_out_ref), (step_hbm, sizes.at[me])])]
    for copy in loads:
        copy.start()

    def up(xt):
        return lax.dot_general(xt.astype(BF16), w_in_ref[...], (((0,), (0,)), ((), ())), preferred_element_type=F32)

    def act(p, gain, shift):
        v = p * gain + shift
        return v + v * jnp.tanh(v * (v * v * CUB + LIN))

    def down(h):
        return lax.dot_general(w_out_ref[...], jnp.concatenate(h, axis=0).astype(BF16), (((1,), (1,)), ((), ())), preferred_element_type=F32)

    def unpack(q):
        gains[q, 0] = 0.5 * (1.0 + rows[q, 0].astype(F32))
        gains[q, 1] = 0.5 * rows[q, 1].astype(F32)
        for k in range(steps):
            hs[q, k:k + 1] = jnp.broadcast_to(sizes[q, :, k:k + 1], (1, width))

    for copy in loads:
        copy.wait()
    unpack(me)

    ring = [0] + [d for d in sorted(range(chips), key=lambda d: min(d, chips - d)) if d]
    my_chip, my_core = me // per, lax.rem(me, per)
    sent = []

    def push(src, dst, send_sem, recv_sem, q):
        copy = pltpu.make_async_remote_copy(src, dst, send_sem, recv_sem, device_id={"time": q}, device_id_type=MESH)
        copy.start()
        sent.append(copy)

    pre[0] = up(x_ref[lax.rem(my_chip + ring[0], chips)])
    for i, d in enumerate(ring):
        chip = lax.rem(my_chip + d, chips)
        if i + 1 < chips:
            pre[(i + 1) % 2] = up(x_ref[lax.rem(my_chip + ring[i + 1], chips)])
        p = pre[i % 2]
        for k in range(steps):
            f = down([act(p, gains[me, 0, k:k + 1], gains[me, 1, k:k + 1])])
            for c in range(per):
                first_send[chip * per + c, k] = f[:, c * width:(c + 1) * width] * hs[me, k:k + 1]
        if i == 1:
            pl.semaphore_wait(barrier, n - 1)
            for e in sorted(range(1, n), key=lambda e: (min(e // per, chips - e // per), e)):
                q = lax.rem(my_chip + e // per, chips) * per + lax.rem(my_core + e % per, per)
                push(rows.at[me], rows.at[me], row_send.at[q], row_recv.at[me], q)
                push(sizes.at[me], sizes.at[me], size_send.at[q], size_recv.at[me], q)
        for c in range(per):
            if not (d or c):
                first[me] = first_send[me]
        for e in list(ring[:i + 1] if i == 1 else ring[i:i + 1] if i > 1 else []):
            for c in range(per):
                if e or c:
                    q = lax.rem(my_chip + e, chips) * per + lax.rem(my_core + c, per)
                    push(first_send.at[q], first.at[me], f_send.at[q], f_recv.at[me], q)

    x_mine = x_ref[mine_b, :, mine_l]
    lat[0, 0] = x_mine
    final[0, 0] = x_mine
    here = []

    def need(j):
        while len(here) * steps <= j:
            group = [len(here) + c for c in range(per)]
            for q in group:
                @pl.when(me != q)
                def _():
                    for ref, send_sem, recv_sem in ((rows, row_send, row_recv), (sizes, size_send, size_recv), (first, f_send, f_recv)):
                        pltpu.make_async_remote_copy(ref.at[q], ref.at[q], send_sem.at[q], recv_sem.at[q], device_id={"time": q}, device_id_type=MESH).wait_recv()
            for q in group:
                here.append(q)
                unpack(q)
                for k in range(steps):
                    j0 = q * steps + k
                    if j0 + 1 < total:
                        lat[0, j0 + 1] = lat[0, j0] + first[q, k]
                    if not j0:
                        for s in range(1, SWEEPS - 1):
                            lat[s, 1] = lat[0, 1]
                        final[0, 1] = lat[0, 1]

    def send(lo, hi):
        q, a, b = lo // steps, lo % steps, hi - lo // steps * steps
        copy = pltpu.make_async_remote_copy(final.at[q, a:b], out_ref.at[a:b, mine_b, :, mine_l], o_send.at[lo], o_recv.at[me, a], device_id={"time": q}, device_id_type=MESH)

        @pl.when(me != q)
        def _():
            copy.start()

        @pl.when(me == q)
        def _():
            for k in range(a, b):
                out_ref[k, mine_b, :, mine_l] = final[q, k]

    def load(item):
        s, j = item
        return jnp.concatenate([lat[s, j], lat[s, j + 1]], axis=1)

    def finish(slot, item):
        s, j = item
        last = s + 2 == SWEEPS
        p = pre[slot]
        pair = [(c, (j + c) // steps, (j + c) % steps) for c in range(2)]
        f = down([act(p[c * width:(c + 1) * width], gains[q, 0, k:k + 1], gains[q, 1, k:k + 1]) for c, q, k in pair])
        for c, q, k in pair:
            nxt = (final[q, k] if last else lat[s + 1, j + c]) + f[:, c * width:(c + 1) * width] * hs[q, k:k + 1]
            if last:
                final[(j + c + 1) // steps, (j + c + 1) % steps] = nxt
            else:
                lat[s + 1, j + c + 1] = nxt
            if s + 1 == j + c:
                final[(j + c + 1) // steps, (j + c + 1) % steps] = nxt

    starts = list(range(1, total - 1, 2))
    items = []
    for t in range(len(starts) + SWEEPS - 2):
        for s in range(SWEEPS - 1):
            if 0 <= t - s < len(starts) and starts[t - s] + 1 > s:
                items.append((s, starts[t - s]))
    cuts = (total - 15, total - 7, total - 5)
    need(items[0][1] + 1)
    pre[0] = up(load(items[0]))
    gone = 0
    sizes_sent = []
    for i, item in enumerate(items):
        if i + 1 < len(items):
            need(items[i + 1][1] + 1)
            pre[(i + 1) % 2] = up(load(items[i + 1]))
        finish(i % 2, item)
        s, j = item
        if s + 2 == SWEEPS and j in cuts or i + 1 == len(items):
            ready = j + 3
            while gone < ready:
                upto = min(ready, (gone // steps + 1) * steps)
                if upto % steps and j not in cuts[-1:] and i + 1 < len(items):
                    break
                send(gone, upto)
                sizes_sent.append((gone, upto))
                gone = upto

    for copy in sent:
        copy.wait_send()
    for lo, hi in sizes_sent:
        q, a, b = lo // steps, lo % steps, hi - lo // steps * steps

        @pl.when(me != q)
        def _():
            pltpu.make_async_remote_copy(final.at[q, a:b], out_ref.at[a:b, mine_b, :, mine_l], o_send.at[lo], o_recv.at[me, a], device_id={"time": q}, device_id_type=MESH).wait_send()

        @pl.when(me == q)
        def _():
            for d in range(1, n):
                src = lax.rem(me + d, n)
                src_l = pl.ds(pl.multiple_of(lax.rem(src, per) * width, width), width)
                pltpu.make_async_remote_copy(final.at[q, a:b], out_ref.at[a:b, src // per, :, src_l], o_send.at[lo], o_recv.at[src, a], device_id={"time": src}, device_id_type=MESH).wait_recv()


def solution(mesh):
    n = mesh.shape["time"]

    def per_device(x_init, w_in, w_out, mod_scale, mod_shift, step_size):
        samples, tokens, chans = x_init.shape
        hidden = w_in.shape[1]
        steps = step_size.shape[0]
        total = n * steps
        width = samples * tokens // n
        anywhere = pl.BlockSpec(memory_space=pl.ANY)
        dma = pltpu.SemaphoreType.DMA
        out = pl.pallas_call(
            functools.partial(kernel, n),
            out_shape=pltpu.VMEM((steps, samples, chans, tokens), F32),
            in_specs=[anywhere] * 6,
            out_specs=pl.BlockSpec(memory_space=pltpu.VMEM),
            scratch_shapes=[
                pltpu.VMEM((samples, chans, tokens), F32),
                pltpu.VMEM((chans, hidden), BF16),
                pltpu.VMEM((chans, hidden), BF16),
                pltpu.VMEM((n, 2, steps, hidden), BF16),
                pltpu.VMEM((n, 1, steps), F32),
                pltpu.VMEM((n, 2, steps, hidden), F32),
                pltpu.VMEM((n, steps, width), F32),
                pltpu.VMEM((n, steps, chans, width), F32),
                pltpu.VMEM((n, steps, chans, width), F32),
                pltpu.VMEM((SWEEPS - 1, total, chans, width), F32),
                pltpu.VMEM((n, steps, chans, width), F32),
                pltpu.VMEM((2, 2 * width, hidden), F32),
                dma((6,)), dma((n,)), dma((n,)), dma((n,)), dma((n,)), dma((n,)), dma((n,)), dma((total,)), dma((n, steps)),
            ],
            compiler_params=pltpu.CompilerParams(collective_id=0, has_side_effects=True),
        )(jnp.transpose(x_init, (0, 2, 1)), w_in, w_out.T, mod_scale, mod_shift, step_size[None])
        return jnp.transpose(out, (0, 1, 3, 2))

    return jax.shard_map(per_device, mesh=mesh, in_specs=(P('data'), P(), P(), P('time'), P('time'), P('time')), out_specs=P('time', 'data'), check_vma=False)
```

```python
import functools

import jax
import jax.numpy as jnp
from jax import lax
from jax.experimental import pallas as pl
from jax.experimental.pallas import tpu as pltpu
from jax.sharding import PartitionSpec as P

SWEEPS = 4
F32, BF16 = jnp.float32, jnp.bfloat16
MESH = pl.DeviceIdType.MESH
LIN = 2 * 0.7978845608028654
CUB = 8 * 0.7978845608028654 * 0.044715


def kernel(n, x_hbm, w_in_hbm, w_out_hbm, scale_hbm, shift_hbm, step_hbm, out_ref,
           x_ref, w_in_ref, w_out_ref, rows, sizes, gains, hs, first, first_send, lat, final, pre,
           load_sem, row_send, row_recv, size_send, size_recv, f_send, f_recv, o_send, o_recv):
    me = lax.axis_index("time")
    steps = scale_hbm.shape[0]
    total = n * steps
    samples, chans, tokens = x_hbm.shape
    width = samples * tokens // n
    per = tokens // width
    chips = n // per

    barrier = pltpu.get_barrier_semaphore()
    for d in range(1, n):
        pl.semaphore_signal(barrier, inc=1, device_id={"time": lax.rem(me + d, n)}, device_id_type=MESH)

    mine_b, mine_l = me // per, pl.ds(pl.multiple_of(lax.rem(me, per) * width, width), width)
    loads = [pltpu.make_async_copy(src, dst, load_sem.at[i]) for i, (src, dst) in enumerate([
        (scale_hbm, rows.at[me, 0]), (shift_hbm, rows.at[me, 1]), (x_hbm, x_ref), (w_in_hbm, w_in_ref), (w_out_hbm, w_out_ref), (step_hbm, sizes.at[me])])]
    for copy in loads:
        copy.start()

    def up(xt):
        return lax.dot_general(xt.astype(BF16), w_in_ref[...], (((0,), (0,)), ((), ())), preferred_element_type=F32)

    def act(p, gain, shift):
        v = p * gain + shift
        return v + v * jnp.tanh(v * (v * v * CUB + LIN))

    def down(h):
        return lax.dot_general(w_out_ref[...], jnp.concatenate(h, axis=0).astype(BF16), (((1,), (1,)), ((), ())), preferred_element_type=F32)

    def unpack(q):
        gains[q, 0] = 0.5 * (1.0 + rows[q, 0].astype(F32))
        gains[q, 1] = 0.5 * rows[q, 1].astype(F32)
        for k in range(steps):
            hs[q, k:k + 1] = jnp.broadcast_to(sizes[q, :, k:k + 1], (1, width))

    for copy in loads:
        copy.wait()
    unpack(me)

    ring = [0] + [d for d in sorted(range(chips), key=lambda d: min(d, chips - d)) if d]
    my_chip, my_core = me // per, lax.rem(me, per)
    sent = []

    def push(src, dst, send_sem, recv_sem, q):
        copy = pltpu.make_async_remote_copy(src, dst, send_sem, recv_sem, device_id={"time": q}, device_id_type=MESH)
        copy.start()
        sent.append(copy)

    pre[0] = up(x_ref[lax.rem(my_chip + ring[0], chips)])
    for i, d in enumerate(ring):
        chip = lax.rem(my_chip + d, chips)
        if i + 1 < chips:
            pre[(i + 1) % 2] = up(x_ref[lax.rem(my_chip + ring[i + 1], chips)])
        p = pre[i % 2]
        for k in range(steps):
            f = down([act(p, gains[me, 0, k:k + 1], gains[me, 1, k:k + 1])])
            for c in range(per):
                first_send[chip * per + c, k] = f[:, c * width:(c + 1) * width] * hs[me, k:k + 1]
        if i == 1:
            pl.semaphore_wait(barrier, n - 1)
            for e in sorted(range(1, n), key=lambda e: (min(e // per, chips - e // per), e)):
                q = lax.rem(my_chip + e // per, chips) * per + lax.rem(my_core + e % per, per)
                push(rows.at[me], rows.at[me], row_send.at[q], row_recv.at[me], q)
                push(sizes.at[me], sizes.at[me], size_send.at[q], size_recv.at[me], q)
        for c in range(per):
            if not (d or c):
                first[me] = first_send[me]
        for e in list(ring[:i + 1] if i == 1 else ring[i:i + 1] if i > 1 else []):
            for c in range(per):
                if e or c:
                    q = lax.rem(my_chip + e, chips) * per + lax.rem(my_core + c, per)
                    push(first_send.at[q], first.at[me], f_send.at[q], f_recv.at[me], q)

    x_mine = x_ref[mine_b, :, mine_l]
    lat[0, 0] = x_mine
    final[0, 0] = x_mine
    here = []

    def need(j):
        while len(here) * steps <= j:
            group = [len(here) + c for c in range(per)]
            for q in group:
                @pl.when(me != q)
                def _():
                    for ref, send_sem, recv_sem in ((rows, row_send, row_recv), (sizes, size_send, size_recv), (first, f_send, f_recv)):
                        pltpu.make_async_remote_copy(ref.at[q], ref.at[q], send_sem.at[q], recv_sem.at[q], device_id={"time": q}, device_id_type=MESH).wait_recv()
            for q in group:
                here.append(q)
                unpack(q)
                for k in range(steps):
                    j0 = q * steps + k
                    if j0 + 1 < total:
                        lat[0, j0 + 1] = lat[0, j0] + first[q, k]
                    if not j0:
                        for s in range(1, SWEEPS - 1):
                            lat[s, 1] = lat[0, 1]
                        final[0, 1] = lat[0, 1]

    def send(lo, hi):
        q, a, b = lo // steps, lo % steps, hi - lo // steps * steps
        copy = pltpu.make_async_remote_copy(final.at[q, a:b], out_ref.at[a:b, mine_b, :, mine_l], o_send.at[lo], o_recv.at[me, a], device_id={"time": q}, device_id_type=MESH)

        @pl.when(me != q)
        def _():
            copy.start()

        @pl.when(me == q)
        def _():
            for k in range(a, b):
                out_ref[k, mine_b, :, mine_l] = final[q, k]

    def load(item):
        s, j = item
        return jnp.concatenate([lat[s, j], lat[s, j + 1]], axis=1)

    def finish(slot, item):
        s, j = item
        last = s + 2 == SWEEPS
        p = pre[slot]
        pair = [(c, (j + c) // steps, (j + c) % steps) for c in range(2)]
        f = down([act(p[c * width:(c + 1) * width], gains[q, 0, k:k + 1], gains[q, 1, k:k + 1]) for c, q, k in pair])
        for c, q, k in pair:
            nxt = (final[q, k] if last else lat[s + 1, j + c]) + f[:, c * width:(c + 1) * width] * hs[q, k:k + 1]
            if last:
                final[(j + c + 1) // steps, (j + c + 1) % steps] = nxt
            else:
                lat[s + 1, j + c + 1] = nxt
            if j + c == s + 1:
                if not last:
                    final[(j + c + 1) // steps, (j + c + 1) % steps] = nxt
                if s + 2 < SWEEPS - 1:
                    lat[s + 2, j + c + 1] = nxt

    items = [(s - 1, s + 2 * (t - s)) for t in range(total) for s in range(1, SWEEPS) if 0 <= t - s < (total - SWEEPS) // 2]
    cuts = (total - 15, total - 7, total - 5)
    need(items[0][1] + 1)
    pre[0] = up(load(items[0]))
    gone = 0
    sizes_sent = []
    for i, item in enumerate(items):
        if i + 1 < len(items):
            need(items[i + 1][1] + 1)
            pre[(i + 1) % 2] = up(load(items[i + 1]))
        finish(i % 2, item)
        s, j = item
        if s + 2 == SWEEPS and j in cuts or i + 1 == len(items):
            ready = j + 3
            while gone < ready:
                upto = min(ready, (gone // steps + 1) * steps)
                if upto % steps and j not in cuts[-1:] and i + 1 < len(items):
                    break
                send(gone, upto)
                sizes_sent.append((gone, upto))
                gone = upto

    for copy in sent:
        copy.wait_send()
    for lo, hi in sizes_sent:
        q, a, b = lo // steps, lo % steps, hi - lo // steps * steps

        @pl.when(me != q)
        def _():
            pltpu.make_async_remote_copy(final.at[q, a:b], out_ref.at[a:b, mine_b, :, mine_l], o_send.at[lo], o_recv.at[me, a], device_id={"time": q}, device_id_type=MESH).wait_send()

        @pl.when(me == q)
        def _():
            for d in range(1, n):
                src = lax.rem(me + d, n)
                src_l = pl.ds(pl.multiple_of(lax.rem(src, per) * width, width), width)
                pltpu.make_async_remote_copy(final.at[q, a:b], out_ref.at[a:b, src // per, :, src_l], o_send.at[lo], o_recv.at[src, a], device_id={"time": src}, device_id_type=MESH).wait_recv()


def solution(mesh):
    n = mesh.shape["time"]

    def per_device(x_init, w_in, w_out, mod_scale, mod_shift, step_size):
        samples, tokens, chans = x_init.shape
        hidden = w_in.shape[1]
        steps = step_size.shape[0]
        total = n * steps
        width = samples * tokens // n
        anywhere = pl.BlockSpec(memory_space=pl.ANY)
        dma = pltpu.SemaphoreType.DMA
        out = pl.pallas_call(
            functools.partial(kernel, n),
            out_shape=pltpu.VMEM((steps, samples, chans, tokens), F32),
            in_specs=[anywhere] * 6,
            out_specs=pl.BlockSpec(memory_space=pltpu.VMEM),
            scratch_shapes=[
                pltpu.VMEM((samples, chans, tokens), F32),
                pltpu.VMEM((chans, hidden), BF16),
                pltpu.VMEM((chans, hidden), BF16),
                pltpu.VMEM((n, 2, steps, hidden), BF16),
                pltpu.VMEM((n, 1, steps), F32),
                pltpu.VMEM((n, 2, steps, hidden), F32),
                pltpu.VMEM((n, steps, width), F32),
                pltpu.VMEM((n, steps, chans, width), F32),
                pltpu.VMEM((n, steps, chans, width), F32),
                pltpu.VMEM((SWEEPS - 1, total, chans, width), F32),
                pltpu.VMEM((n, steps, chans, width), F32),
                pltpu.VMEM((2, 2 * width, hidden), F32),
                dma((6,)), dma((n,)), dma((n,)), dma((n,)), dma((n,)), dma((n,)), dma((n,)), dma((total,)), dma((n, steps)),
            ],
            compiler_params=pltpu.CompilerParams(collective_id=0, has_side_effects=True),
        )(jnp.transpose(x_init, (0, 2, 1)), w_in, w_out.T, mod_scale, mod_shift, step_size[None])
        return jnp.transpose(out, (0, 1, 3, 2))

    return jax.shard_map(per_device, mesh=mesh, in_specs=(P('data'), P(), P(), P('time'), P('time'), P('time')), out_specs=P('time', 'data'), check_vma=False)
```

```python
import functools

import jax
import jax.numpy as jnp
from jax import lax
from jax.experimental import pallas as pl
from jax.experimental.pallas import tpu as pltpu
from jax.sharding import PartitionSpec as P

SWEEPS = 4
F32, BF16 = jnp.float32, jnp.bfloat16
MESH = pl.DeviceIdType.MESH
LIN = 2 * 0.7978845608028654
CUB = 8 * 0.7978845608028654 * 0.044715


def kernel(n, x_hbm, w_in_hbm, w_out_hbm, scale_hbm, shift_hbm, step_hbm, out_ref,
           x_ref, w_in_ref, w_out_ref, rows, sizes, gains, hs, first, first_send, lat, final, pre,
           load_sem, row_send, row_recv, size_send, size_recv, f_send, f_recv, o_send, o_recv):
    me = lax.axis_index("time")
    steps = scale_hbm.shape[0]
    total = n * steps
    samples, chans, tokens = x_hbm.shape
    width = samples * tokens // n
    per = tokens // width
    chips = n // per

    barrier = pltpu.get_barrier_semaphore()
    for d in range(1, n):
        pl.semaphore_signal(barrier, inc=1, device_id={"time": lax.rem(me + d, n)}, device_id_type=MESH)

    mine_b, mine_l = me // per, pl.ds(pl.multiple_of(lax.rem(me, per) * width, width), width)
    loads = [pltpu.make_async_copy(src, dst, load_sem.at[i]) for i, (src, dst) in enumerate([
        (scale_hbm, rows.at[me, 0]), (shift_hbm, rows.at[me, 1]), (x_hbm, x_ref), (w_in_hbm, w_in_ref), (w_out_hbm, w_out_ref), (step_hbm, sizes.at[me])])]
    for copy in loads:
        copy.start()

    def up(xt):
        return lax.dot_general(xt.astype(BF16), w_in_ref[...], (((0,), (0,)), ((), ())), preferred_element_type=F32)

    def act(p, gain, shift):
        v = p * gain + shift
        return v + v * jnp.tanh(v * (v * v * CUB + LIN))

    def down(h):
        return lax.dot_general(w_out_ref[...], jnp.concatenate(h, axis=0).astype(BF16), (((1,), (1,)), ((), ())), preferred_element_type=F32)

    def unpack(q):
        gains[q, 0] = 0.5 * (1.0 + rows[q, 0].astype(F32))
        gains[q, 1] = 0.5 * rows[q, 1].astype(F32)
        for k in range(steps):
            hs[q, k:k + 1] = jnp.broadcast_to(sizes[q, :, k:k + 1], (1, width))

    for copy in loads:
        copy.wait()
    unpack(me)

    ring = [0] + [d for d in sorted(range(chips), key=lambda d: min(d, chips - d)) if d]
    my_chip, my_core = me // per, lax.rem(me, per)
    sent = []

    def push(src, dst, send_sem, recv_sem, q):
        copy = pltpu.make_async_remote_copy(src, dst, send_sem, recv_sem, device_id={"time": q}, device_id_type=MESH)
        copy.start()
        sent.append(copy)

    pre[0] = up(x_ref[lax.rem(my_chip + ring[0], chips)])
    for i, d in enumerate(ring):
        chip = lax.rem(my_chip + d, chips)
        if i + 1 < chips:
            pre[(i + 1) % 2] = up(x_ref[lax.rem(my_chip + ring[i + 1], chips)])
        p = pre[i % 2]
        for k in range(steps):
            f = down([act(p, gains[me, 0, k:k + 1], gains[me, 1, k:k + 1])])
            for c in range(per):
                first_send[chip * per + c, k] = f[:, c * width:(c + 1) * width] * hs[me, k:k + 1]
        if i == 1:
            pl.semaphore_wait(barrier, n - 1)
            for e in sorted(range(1, n), key=lambda e: (min(e // per, chips - e // per), e)):
                q = lax.rem(my_chip + e // per, chips) * per + lax.rem(my_core + e % per, per)
                push(rows.at[me], rows.at[me], row_send.at[q], row_recv.at[me], q)
                push(sizes.at[me], sizes.at[me], size_send.at[q], size_recv.at[me], q)
        for c in range(per):
            if not (d or c):
                first[me] = first_send[me]
        for e in list(ring[:i + 1] if i == 1 else ring[i:i + 1] if i > 1 else []):
            for c in range(per):
                if e or c:
                    q = lax.rem(my_chip + e, chips) * per + lax.rem(my_core + c, per)
                    push(first_send.at[q], first.at[me], f_send.at[q], f_recv.at[me], q)

    x_mine = x_ref[mine_b, :, mine_l]
    lat[0, 0] = x_mine
    final[0, 0] = x_mine
    here = []

    def need(j):
        while len(here) * steps <= j:
            group = [len(here) + c for c in range(per if len(here) < 2 * per else n - 2 * per)]
            for q in group:
                @pl.when(me != q)
                def _():
                    for ref, send_sem, recv_sem in ((rows, row_send, row_recv), (sizes, size_send, size_recv), (first, f_send, f_recv)):
                        pltpu.make_async_remote_copy(ref.at[q], ref.at[q], send_sem.at[q], recv_sem.at[q], device_id={"time": q}, device_id_type=MESH).wait_recv()
            for q in group:
                here.append(q)
                unpack(q)
                for k in range(steps):
                    j0 = q * steps + k
                    if j0 + 1 < total:
                        lat[0, j0 + 1] = lat[0, j0] + first[q, k]
                    if not j0:
                        for s in range(1, SWEEPS - 1):
                            lat[s, 1] = lat[0, 1]
                        final[0, 1] = lat[0, 1]

    def send(lo, hi):
        q, a, b = lo // steps, lo % steps, hi - lo // steps * steps
        copy = pltpu.make_async_remote_copy(final.at[q, a:b], out_ref.at[a:b, mine_b, :, mine_l], o_send.at[lo], o_recv.at[me, a], device_id={"time": q}, device_id_type=MESH)

        @pl.when(me != q)
        def _():
            copy.start()

    def load(item):
        s, j = item
        return jnp.concatenate([lat[s, j], lat[s, j + 1]], axis=1)

    def finish(slot, item):
        s, j = item
        last = s + 2 == SWEEPS
        p = pre[slot]
        pair = [(c, (j + c) // steps, (j + c) % steps) for c in range(2)]
        f = down([act(p[c * width:(c + 1) * width], gains[q, 0, k:k + 1], gains[q, 1, k:k + 1]) for c, q, k in pair])
        for c, q, k in pair:
            nxt = (final[q, k] if last else lat[s + 1, j + c]) + f[:, c * width:(c + 1) * width] * hs[q, k:k + 1]
            if last:
                final[(j + c + 1) // steps, (j + c + 1) % steps] = nxt
            else:
                lat[s + 1, j + c + 1] = nxt
            if j + c == s + 1:
                if not last:
                    final[(j + c + 1) // steps, (j + c + 1) % steps] = nxt
                if s + 2 < SWEEPS - 1:
                    lat[s + 2, j + c + 1] = nxt

    items = [(s - 1, s + 2 * (t - s)) for t in range(total) for s in range(1, SWEEPS) if 0 <= t - s < (total - SWEEPS) // 2]
    cuts = (total - 15, total - 7)
    need(items[0][1] + 1)
    pre[0] = up(load(items[0]))
    gone = 0
    sizes_sent = []
    for i, item in enumerate(items):
        if i + 1 < len(items):
            need(items[i + 1][1] + 1)
            pre[(i + 1) % 2] = up(load(items[i + 1]))
        finish(i % 2, item)
        s, j = item
        if s + 2 == SWEEPS and j in cuts or i + 1 == len(items):
            ready = j + 3
            while gone < ready:
                upto = min(ready, (gone // steps + 1) * steps)
                if upto % steps and j not in cuts[-1:] and i + 1 < len(items):
                    break
                send(gone, upto)
                sizes_sent.append((gone, upto))
                gone = upto

    for k in range(steps):
        out_ref[k, mine_b, :, mine_l] = final[me, k]
    for copy in sent:
        copy.wait_send()
    for lo, hi in sizes_sent:
        q, a, b = lo // steps, lo % steps, hi - lo // steps * steps

        @pl.when(me != q)
        def _():
            pltpu.make_async_remote_copy(final.at[q, a:b], out_ref.at[a:b, mine_b, :, mine_l], o_send.at[lo], o_recv.at[me, a], device_id={"time": q}, device_id_type=MESH).wait_send()

        @pl.when(me == q)
        def _():
            for d in range(1, n):
                src = lax.rem(me + d, n)
                src_l = pl.ds(pl.multiple_of(lax.rem(src, per) * width, width), width)
                pltpu.make_async_remote_copy(final.at[q, a:b], out_ref.at[a:b, src // per, :, src_l], o_send.at[lo], o_recv.at[src, a], device_id={"time": src}, device_id_type=MESH).wait_recv()


def solution(mesh):
    n = mesh.shape["time"]

    def per_device(x_init, w_in, w_out, mod_scale, mod_shift, step_size):
        samples, tokens, chans = x_init.shape
        hidden = w_in.shape[1]
        steps = step_size.shape[0]
        total = n * steps
        width = samples * tokens // n
        anywhere = pl.BlockSpec(memory_space=pl.ANY)
        dma = pltpu.SemaphoreType.DMA
        out = pl.pallas_call(
            functools.partial(kernel, n),
            out_shape=pltpu.VMEM((steps, samples, chans, tokens), F32),
            in_specs=[anywhere] * 6,
            out_specs=pl.BlockSpec(memory_space=pltpu.VMEM),
            scratch_shapes=[
                pltpu.VMEM((samples, chans, tokens), F32),
                pltpu.VMEM((chans, hidden), BF16),
                pltpu.VMEM((chans, hidden), BF16),
                pltpu.VMEM((n, 2, steps, hidden), BF16),
                pltpu.VMEM((n, 1, steps), F32),
                pltpu.VMEM((n, 2, steps, hidden), F32),
                pltpu.VMEM((n, steps, width), F32),
                pltpu.VMEM((n, steps, chans, width), F32),
                pltpu.VMEM((n, steps, chans, width), F32),
                pltpu.VMEM((SWEEPS - 1, total, chans, width), F32),
                pltpu.VMEM((n, steps, chans, width), F32),
                pltpu.VMEM((2, 2 * width, hidden), F32),
                dma((6,)), dma((n,)), dma((n,)), dma((n,)), dma((n,)), dma((n,)), dma((n,)), dma((total,)), dma((n, steps)),
            ],
            compiler_params=pltpu.CompilerParams(collective_id=0, has_side_effects=True),
        )(jnp.transpose(x_init, (0, 2, 1)), w_in, w_out.T, mod_scale, mod_shift, step_size[None])
        return jnp.transpose(out, (0, 1, 3, 2))

    return jax.shard_map(per_device, mesh=mesh, in_specs=(P('data'), P(), P(), P('time'), P('time'), P('time')), out_specs=P('time', 'data'), check_vma=False)
```

```python
import functools

import jax
import jax.numpy as jnp
from jax import lax
from jax.experimental import pallas as pl
from jax.experimental.pallas import tpu as pltpu
from jax.sharding import PartitionSpec as P

SWEEPS = 4
F32, BF16 = jnp.float32, jnp.bfloat16
MESH = pl.DeviceIdType.MESH
LIN = 2 * 0.7978845608028654
CUB = 8 * 0.7978845608028654 * 0.044715


def kernel(n, x_hbm, w_in_hbm, w_out_hbm, scale_hbm, shift_hbm, step_hbm, out_ref,
           x_ref, w_in_ref, w_out_ref, rows, sizes, gains, hs, first, first_send, lat, final, pre,
           load_sem, row_send, row_recv, size_send, size_recv, f_send, f_recv, o_send, o_recv):
    me = lax.axis_index("time")
    steps = scale_hbm.shape[0]
    total = n * steps
    samples, chans, tokens = x_hbm.shape
    width = samples * tokens // n
    per = tokens // width
    chips = n // per

    barrier = pltpu.get_barrier_semaphore()
    for d in range(1, n):
        pl.semaphore_signal(barrier, inc=1, device_id={"time": lax.rem(me + d, n)}, device_id_type=MESH)

    mine_b, mine_l = me // per, pl.ds(pl.multiple_of(lax.rem(me, per) * width, width), width)
    loads = [pltpu.make_async_copy(src, dst, load_sem.at[i]) for i, (src, dst) in enumerate([
        (scale_hbm, rows.at[me, 0]), (shift_hbm, rows.at[me, 1]), (x_hbm, x_ref), (w_in_hbm, w_in_ref), (w_out_hbm, w_out_ref), (step_hbm, sizes.at[me])])]
    for copy in loads:
        copy.start()

    def up(xt):
        return lax.dot_general(xt.astype(BF16), w_in_ref[...], (((0,), (0,)), ((), ())), preferred_element_type=F32)

    def act(p, gain, shift):
        v = p * gain + shift
        return v + v * jnp.tanh(v * (v * v * CUB + LIN))

    def down(h):
        return lax.dot_general(w_out_ref[...], jnp.concatenate(h, axis=0).astype(BF16), (((1,), (1,)), ((), ())), preferred_element_type=F32)

    def unpack(q):
        gains[q, 0] = 0.5 * (1.0 + rows[q, 0].astype(F32))
        gains[q, 1] = 0.5 * rows[q, 1].astype(F32)
        for k in range(steps):
            hs[q, k:k + 1] = jnp.broadcast_to(sizes[q, :, k:k + 1], (1, width))

    for copy in loads[2:4]:
        copy.wait()

    ring = [0] + [d for d in sorted(range(chips), key=lambda d: min(d, chips - d)) if d]
    my_chip, my_core = me // per, lax.rem(me, per)
    sent = []

    def push(src, dst, send_sem, recv_sem, q):
        copy = pltpu.make_async_remote_copy(src, dst, send_sem, recv_sem, device_id={"time": q}, device_id_type=MESH)
        copy.start()
        sent.append(copy)

    pre[0] = up(x_ref[lax.rem(my_chip + ring[0], chips)])
    for copy in loads[:2] + loads[4:]:
        copy.wait()
    unpack(me)
    for i, d in enumerate(ring):
        chip = lax.rem(my_chip + d, chips)
        if i + 1 < chips:
            pre[(i + 1) % 2] = up(x_ref[lax.rem(my_chip + ring[i + 1], chips)])
        p = pre[i % 2]
        for k in range(steps):
            f = down([act(p, gains[me, 0, k:k + 1], gains[me, 1, k:k + 1])])
            for c in range(per):
                first_send[chip * per + c, k] = f[:, c * width:(c + 1) * width] * hs[me, k:k + 1]
        if i == 1:
            pl.semaphore_wait(barrier, n - 1)
            for e in sorted(range(1, n), key=lambda e: (min(e // per, chips - e // per), e)):
                q = lax.rem(my_chip + e // per, chips) * per + lax.rem(my_core + e % per, per)
                push(rows.at[me], rows.at[me], row_send.at[q], row_recv.at[me], q)
                push(sizes.at[me], sizes.at[me], size_send.at[q], size_recv.at[me], q)
        for c in range(per):
            if not (d or c):
                first[me] = first_send[me]
        for e in list(ring[:i + 1] if i == 1 else ring[i:i + 1] if i > 1 else []):
            for c in range(per):
                if e or c:
                    q = lax.rem(my_chip + e, chips) * per + lax.rem(my_core + c, per)
                    push(first_send.at[q], first.at[me], f_send.at[q], f_recv.at[me], q)

    x_mine = x_ref[mine_b, :, mine_l]
    lat[0, 0] = x_mine
    final[0, 0] = x_mine
    here = []

    def need(j):
        while len(here) * steps <= j:
            group = [len(here) + c for c in range(per if len(here) < 2 * per else n - 2 * per)]
            for q in group:
                @pl.when(me != q)
                def _():
                    for ref, send_sem, recv_sem in ((rows, row_send, row_recv), (sizes, size_send, size_recv), (first, f_send, f_recv)):
                        pltpu.make_async_remote_copy(ref.at[q], ref.at[q], send_sem.at[q], recv_sem.at[q], device_id={"time": q}, device_id_type=MESH).wait_recv()
            for q in group:
                here.append(q)
                unpack(q)
                for k in range(steps):
                    j0 = q * steps + k
                    if j0 + 1 < total:
                        lat[0, j0 + 1] = lat[0, j0] + first[q, k]
                    if not j0:
                        for s in range(1, SWEEPS - 1):
                            lat[s, 1] = lat[0, 1]
                        final[0, 1] = lat[0, 1]

    def send(lo, hi):
        q, a, b = lo // steps, lo % steps, hi - lo // steps * steps
        copy = pltpu.make_async_remote_copy(final.at[q, a:b], out_ref.at[a:b, mine_b, :, mine_l], o_send.at[lo], o_recv.at[me, a], device_id={"time": q}, device_id_type=MESH)

        @pl.when(me != q)
        def _():
            copy.start()

    def load(item):
        s, j = item
        return jnp.concatenate([lat[s, j], lat[s, j + 1]], axis=1)

    def finish(slot, item):
        s, j = item
        last = s + 2 == SWEEPS
        p = pre[slot]
        pair = [(c, (j + c) // steps, (j + c) % steps) for c in range(2)]
        f = down([act(p[c * width:(c + 1) * width], gains[q, 0, k:k + 1], gains[q, 1, k:k + 1]) for c, q, k in pair])
        for c, q, k in pair:
            nxt = (final[q, k] if last else lat[s + 1, j + c]) + f[:, c * width:(c + 1) * width] * hs[q, k:k + 1]
            if last:
                final[(j + c + 1) // steps, (j + c + 1) % steps] = nxt
            else:
                lat[s + 1, j + c + 1] = nxt
            if j + c == s + 1:
                if not last:
                    final[(j + c + 1) // steps, (j + c + 1) % steps] = nxt
                if s + 2 < SWEEPS - 1:
                    lat[s + 2, j + c + 1] = nxt

    items = [(s - 1, s + 2 * (t - s)) for t in range(total) for s in range(1, SWEEPS) if 0 <= t - s < (total - SWEEPS) // 2]
    cuts = (total - 15, total - 7)
    need(items[0][1] + 1)
    pre[0] = up(load(items[0]))
    gone = 0
    sizes_sent = []
    for i, item in enumerate(items):
        if i + 1 < len(items):
            need(items[i + 1][1] + 1)
            pre[(i + 1) % 2] = up(load(items[i + 1]))
        finish(i % 2, item)
        s, j = item
        if s + 2 == SWEEPS and j in cuts or i + 1 == len(items):
            ready = j + 3
            while gone < ready:
                upto = min(ready, (gone // steps + 1) * steps)
                if upto % steps and j not in cuts[-1:] and i + 1 < len(items):
                    break
                send(gone, upto)
                sizes_sent.append((gone, upto))
                gone = upto

    for k in range(steps):
        out_ref[k, mine_b, :, mine_l] = final[me, k]
    for copy in sent:
        copy.wait_send()
    for lo, hi in sizes_sent:
        q, a, b = lo // steps, lo % steps, hi - lo // steps * steps

        @pl.when(me != q)
        def _():
            pltpu.make_async_remote_copy(final.at[q, a:b], out_ref.at[a:b, mine_b, :, mine_l], o_send.at[lo], o_recv.at[me, a], device_id={"time": q}, device_id_type=MESH).wait_send()

        @pl.when(me == q)
        def _():
            for d in range(1, n):
                src = lax.rem(me + d, n)
                src_l = pl.ds(pl.multiple_of(lax.rem(src, per) * width, width), width)
                pltpu.make_async_remote_copy(final.at[q, a:b], out_ref.at[a:b, src // per, :, src_l], o_send.at[lo], o_recv.at[src, a], device_id={"time": src}, device_id_type=MESH).wait_recv()


def solution(mesh):
    n = mesh.shape["time"]

    def per_device(x_init, w_in, w_out, mod_scale, mod_shift, step_size):
        samples, tokens, chans = x_init.shape
        hidden = w_in.shape[1]
        steps = step_size.shape[0]
        total = n * steps
        width = samples * tokens // n
        anywhere = pl.BlockSpec(memory_space=pl.ANY)
        dma = pltpu.SemaphoreType.DMA
        out = pl.pallas_call(
            functools.partial(kernel, n),
            out_shape=pltpu.VMEM((steps, samples, chans, tokens), F32),
            in_specs=[anywhere] * 6,
            out_specs=pl.BlockSpec(memory_space=pltpu.VMEM),
            scratch_shapes=[
                pltpu.VMEM((samples, chans, tokens), F32),
                pltpu.VMEM((chans, hidden), BF16),
                pltpu.VMEM((chans, hidden), BF16),
                pltpu.VMEM((n, 2, steps, hidden), BF16),
                pltpu.VMEM((n, 1, steps), F32),
                pltpu.VMEM((n, 2, steps, hidden), F32),
                pltpu.VMEM((n, steps, width), F32),
                pltpu.VMEM((n, steps, chans, width), F32),
                pltpu.VMEM((n, steps, chans, width), F32),
                pltpu.VMEM((SWEEPS - 1, total, chans, width), F32),
                pltpu.VMEM((n, steps, chans, width), F32),
                pltpu.VMEM((2, 2 * width, hidden), F32),
                dma((6,)), dma((n,)), dma((n,)), dma((n,)), dma((n,)), dma((n,)), dma((n,)), dma((total,)), dma((n, steps)),
            ],
            compiler_params=pltpu.CompilerParams(collective_id=0, has_side_effects=True),
        )(jnp.transpose(x_init, (0, 2, 1)), w_in, w_out.T, mod_scale, mod_shift, step_size[None])
        return jnp.transpose(out, (0, 1, 3, 2))

    return jax.shard_map(per_device, mesh=mesh, in_specs=(P('data'), P(), P(), P('time'), P('time'), P('time')), out_specs=P('time', 'data'), check_vma=False)
```
